1024 devices in a mesh: wide: 16 (over y_hi, x), narrow: 64 (over z, y_lo, core).
Axes of the slice: x: 4, y: 8 (y_hi: 4, y_lo: 2; y = y_hi * 2 + y_lo), z: 16, core: 2. Of those that a mesh axis runs over, the one named last changes fastest.
Arguments:
- flow_field: float32 [12, 256, 512, 128], P(None, 'wide', 'narrow'), may hold values from -4 to 4
- offsets: float32 [32768, 3, 256], P(('wide', 'narrow')), may hold values from 0 to 1
- cells_first: int32 [32768, 3], P(('wide', 'narrow')), may hold values from 0 to 511, as said below
- cells_second: int32 [32768, 3], P(('wide', 'narrow')), may hold values from 0 to 511, as said below
- live_counts: int32 [1024], P(('wide', 'narrow')), may hold values from 1 to 32, as said below
- destination: int32 [32768, 1], P(('wide', 'narrow')), may hold values from 0 to 63; in each aligned block of 32 rows (0 to 31, 32 to 63, ...) at most 4 rows name the same one
Outputs:
- profile: float32 [4, 256], P(None, 'wide')
- tracer_offsets: float32 [262144, 3, 256], P(('wide', 'narrow'))
- tracer_cells: int32 [262144, 3], P(('wide', 'narrow'))
The draws below stay inside these ranges and needn't reach their ends.
Inputs may be any that keep to these rules, and one draw needn't show every extreme that they name: `cells_first`: block slot b belongs to device b // 32; its x index is any cell, its y index lies from 2 below that device's first y cell to 12 above it, modulo 256, and its z index lies from 2 below that device's first z cell to 4 above it, modulo 512. `cells_second`: each entry differs from the same block's cells_first entry by -1, 0 or 1, modulo the extent of that dimension. The first live_counts[d] slots of device d hold live blocks; at least one device has all 32 slots live. Among the 32 slots of one device, live or not, at most 4 name the same destination, and some device reaches 4.
All inputs are finite; a program needn't handle non-finite values.
Results may differ from the reference program's by a relative error of at most 0.0003.
Values sent between devices are 32-bit elements; how exact they have to be, the bound alone decides.
No kernel may reach another device: no remote copies, remote signals or barrier semaphores. Data moves between devices by JAX's collectives and lax.ppermute only.
A program may use at most 64 MiB of HBM per device.

```python
import math
import jax
import jax.numpy as jnp
import numpy as np
from jax import lax

NX = 128
CY = 16
CZ = 8
BLK_DEV = 32
PB = 256
COMP = 12
CAP = 4
NSTAT = 4
NY = 256
NZ = 512
BLOCKS = 32768
SLOTS = 262144
N_WIDE = 16
N_NARROW = 64


def cell_pair(key):
    index_all = jnp.arange(BLOCKS, dtype=jnp.int32)
    device = index_all // BLK_DEV
    narrow_total = NZ // CZ
    low_y = device // narrow_total * CY - 2
    low_z = device % narrow_total * CZ - 2
    cell_x = jax.random.randint(jax.random.fold_in(key, 1), (BLOCKS,), 0, NX, dtype=jnp.int32)
    cell_y = (low_y + jax.random.randint(jax.random.fold_in(key, 2), (BLOCKS,), 0, CY - 1, dtype=jnp.int32)) % NY
    cell_z = (low_z + jax.random.randint(jax.random.fold_in(key, 3), (BLOCKS,), 0, CZ - 1, dtype=jnp.int32)) % NZ
    first_cells = jnp.stack([cell_x, cell_y, cell_z], axis=1)
    moves = jax.random.randint(jax.random.fold_in(key, 4), (BLOCKS, 3), -1, 2, dtype=jnp.int32)
    extents = jnp.array([NX, NY, NZ], dtype=jnp.int32)
    second_cells = (first_cells + moves + extents) % extents
    return (first_cells.astype(jnp.int32), second_cells.astype(jnp.int32))


def draw_cells_first(key, part):
    return cell_pair(jax.random.fold_in(key, 17))[0]


def draw_cells_second(key, part):
    return cell_pair(jax.random.fold_in(key, 17))[1]


def draw_live_counts(key, part):
    devices = BLOCKS // BLK_DEV
    initial_draw = jax.random.randint(jax.random.fold_in(key, 1), (devices,), 1, BLK_DEV + 1, dtype=jnp.int32)
    second_draw = jax.random.randint(jax.random.fold_in(key, 2), (devices,), 1, BLK_DEV + 1, dtype=jnp.int32)
    chosen = jax.random.randint(jax.random.fold_in(key, 3), (), 0, devices, dtype=jnp.int32)
    counted = jnp.minimum(initial_draw, second_draw)
    return jnp.where(jnp.arange(devices, dtype=jnp.int32) == chosen, BLK_DEV, counted).astype(jnp.int32)


def levels(stream_key, dims, split, low, top_value):
    factor_of = 1.0
    for dim, shards_of in split:
        steps = jax.random.uniform(jax.random.fold_in(jax.random.fold_in(stream_key, 6), dim), (shards_of,), jnp.float32, low / len(split), top_value / len(split))
        factor_of = factor_of * jnp.repeat(jnp.exp(steps), dims[dim] // shards_of).reshape((-1,) + (1,) * (len(dims) - 1 - dim))
    return factor_of


def shared_out(rng, own, number, rows, amount, top, reach, lean):
    sequence = jax.random.permutation(rng, amount)
    crowded, ordinary = load_shares(amount, rows * top, reach, lean, True), load_shares(amount, rows * top, reach, lean, False)
    places = jnp.arange(amount)

    def named(sizes, turn):
        used = int((sizes > 0).sum())
        fixed = max(1, used // 4)
        passed = fixed + (places - fixed + turn * (used - fixed)) % max(1, amount - fixed)
        return jnp.zeros((amount,), jnp.int32).at[sequence[jnp.where(places < fixed, places, passed)]].set(jnp.asarray(sizes, jnp.int32))

    sizes = jnp.where(number % 4 == 0, named(crowded, number // 4), named(ordinary, number - number // 4 - 1))
    mixed = jax.random.permutation(jax.random.fold_in(own, 3), amount)
    source_of, taker = mixed[0:amount // 2 * 2:2], mixed[1:amount // 2 * 2:2]
    margin = jnp.minimum(sizes[source_of] - 1, reach - sizes[taker]) // 2
    margin = jnp.where((source_of == sequence[0]) | (taker == sequence[0]) | (sizes[taker] == 0), 0, jnp.maximum(margin, 0))
    passed = jax.random.randint(jax.random.fold_in(own, 4), (amount // 2,), 0, 1 << 20) % (margin + 1)
    sizes = sizes.at[source_of].add(-passed).at[taker].add(passed)
    members = jnp.searchsorted(jnp.cumsum(sizes), jnp.arange(rows * top), side="right").astype(jnp.int32)
    listing = members.reshape(top, rows).T
    listing = listing[jax.random.permutation(jax.random.fold_in(own, 1), rows)]
    turn = jax.random.randint(jax.random.fold_in(own, 2), (rows, 1), 0, top)
    return jnp.take_along_axis(listing, (jnp.arange(top)[None, :] + turn) % top, axis=1)


def load_shares(number_of, total, most, slope, full):
    weights = [(1 << 20) // math.isqrt(grade ** slope) + 1 for grade in range(1, number_of + 1)]
    largest = most if full else min(most, max(-(-total // number_of), total * weights[0] // sum(weights)))
    least = 1 if total - largest >= number_of - 1 else 0
    counts, surplus = [largest] + [least] * (number_of - 1), total - largest - least * (number_of - 1)
    while surplus > 0:
        movable = [i for i in range(1, number_of) if counts[i] < largest] or [i for i in range(1, number_of) if counts[i] < most]
        whole, budget = sum([weights[i] for i in movable]), surplus
        for i in movable:
            more = min(most - counts[i], max(1, budget * weights[i] // whole), surplus)
            counts[i] = counts[i] + more
            surplus = surplus - more
    return np.array(counts)


def normal_values(stream_key, extent, width, reach, split=(), kind=jnp.bfloat16):
    loudness = levels(stream_key, extent, split, -0.22, 0.18) if split else 1.0
    values = jax.random.normal(stream_key, extent, jnp.float32) * width * loudness
    return jnp.minimum(jnp.maximum(values, -reach), reach).astype(kind)


def setup_inputs(seed: int = 0) -> dict:
    key_of = jax.random.split(jax.random.key(seed), 7)
    flow_field = normal_values(key_of[0], (COMP, NY, NZ, NX), 1.0, 4.0, ((1, 16), (2, 64)), jnp.float32)
    offsets = jnp.clip(1.0 * jax.random.uniform(key_of[1], (BLOCKS, 3, PB), jnp.float32) ** levels(key_of[1], (BLOCKS, 3, PB), ((0, 1024),), -0.2, 0.2), 0.0, 1.0)
    cells_first = draw_cells_first(jax.random.fold_in(key_of[6], 71), 0)
    cells_second = draw_cells_second(jax.random.fold_in(key_of[6], 71), 0)
    live_counts = draw_live_counts(jax.random.fold_in(key_of[6], 71), 0)
    destination_keys = jax.random.split(jax.random.fold_in(key_of[5], 1), BLOCKS // BLK_DEV)
    destination_turns = jax.random.permutation(jax.random.fold_in(key_of[5], 3), BLOCKS // BLK_DEV)
    destination = jax.vmap(lambda own, number: shared_out(jax.random.fold_in(key_of[5], 2), own, number, BLK_DEV, N_NARROW, 1, CAP, 2))(destination_keys, destination_turns).reshape((BLOCKS, 1))
    return dict(flow_field=flow_field, offsets=offsets, cells_first=cells_first, cells_second=cells_second, live_counts=live_counts, destination=destination)


time_increment = 0.25


def lagrange(position):
    weights = []
    for node_index in range(6):
        factor = jnp.ones_like(position)
        for other_node in range(6):
            if other_node != node_index:
                factor = factor * ((position - other_node) / (node_index - other_node))
        weights.append(factor)
    return jnp.stack(weights, axis=1)


def interpolate(tile_block, position):
    x_direction_weight = lagrange(position[:, 0])
    weight_y = lagrange(position[:, 1])
    weight_z = lagrange(position[:, 2])
    stencil_points = weight_y[:, :, None, None, :] * weight_z[:, None, :, None, :] * x_direction_weight[:, None, None, :, :]
    stencil_points = stencil_points.reshape(stencil_points.shape[0], 216, stencil_points.shape[-1])
    flat_values = tile_block.reshape(tile_block.shape[0], tile_block.shape[1], 216)
    return jnp.einsum("ikt,itn->ikn", flat_values, stencil_points, precision=lax.Precision.HIGHEST)


def invariants(values):
    gradient = values[:, 3:12].reshape(values.shape[0], 3, 3, values.shape[-1])
    strain = 0.5 * (gradient + jnp.swapaxes(gradient, 1, 2))
    rotation = 0.5 * (gradient - jnp.swapaxes(gradient, 1, 2))
    return jnp.stack([jnp.sum(strain * strain, axis=(1, 2, 3)), jnp.sum(rotation * rotation, axis=(1, 2, 3))], axis=1)


def nearest(difference, extents):
    return (difference + extents // 2) % extents - extents // 2


def reference(flow_field, offsets, cells_first, cells_second, live_counts, destination):
    extents = jnp.array([NX, NY, NZ], dtype=jnp.int32)
    devices = N_WIDE * N_NARROW
    six_steps = jnp.arange(6, dtype=jnp.int32)
    slots_index = jnp.arange(BLK_DEV, dtype=jnp.int32)

    def tiles_of(cells):
        def single(base_cell):
            index_x = (base_cell[0] + six_steps) % NX
            index_y = (base_cell[1] + six_steps) % NY
            index_z = (base_cell[2] + six_steps) % NZ
            return flow_field[:, index_y][:, :, index_z][:, :, :, index_x]
        return jax.vmap(single)(cells)

    def device(packed):
        block_offsets, first_cells, second_cells, target, live_count = packed
        anchor = 2.0 + block_offsets
        early_values = interpolate(tiles_of(first_cells), anchor)
        offset_cells = nearest(first_cells - second_cells, extents).astype(jnp.float32)
        midway = anchor + time_increment * early_values[:, 0:3] + offset_cells[:, :, None]
        later_values = interpolate(tiles_of(second_cells), midway)
        arrived_tracers = anchor + (0.5 * time_increment) * (early_values[:, 0:3] + later_values[:, 0:3])
        living = (slots_index < live_count).astype(jnp.float32)
        statistics = jnp.concatenate([invariants(early_values), invariants(later_values)], axis=1) * living[:, None]
        matching = (target[:, None] == target[None, :]) & (slots_index[None, :] < slots_index[:, None])
        ranking = jnp.sum(matching.astype(jnp.int32), axis=1)
        placing = (target * CAP + ranking).astype(jnp.int32)
        sent_offsets = jnp.zeros((N_NARROW * CAP, 3, PB), jnp.float32).at[placing].set(arrived_tracers * living[:, None, None])
        sent_cells = jnp.full((N_NARROW * CAP, 3), -1, jnp.int32).at[placing].set(jnp.where(living[:, None] > 0, first_cells, -1))
        return statistics, sent_offsets, sent_cells

    statistics, sent_offsets, sent_cells = lax.map(device, (offsets.reshape(devices, BLK_DEV, 3, PB), cells_first.reshape(devices, BLK_DEV, 3), cells_second.reshape(devices, BLK_DEV, 3), destination.reshape(devices, BLK_DEV), live_counts))
    central = ((cells_first[:, 1] + 2) % NY).astype(jnp.int32)
    profile = jax.ops.segment_sum(statistics.reshape(devices * BLK_DEV, NSTAT), central, num_segments=NY).T / (PB * N_NARROW)
    tracer_offsets = jnp.swapaxes(sent_offsets.reshape(N_WIDE, N_NARROW, N_NARROW, CAP, 3, PB), 1, 2).reshape(SLOTS, 3, PB)
    tracer_cells = jnp.swapaxes(sent_cells.reshape(N_WIDE, N_NARROW, N_NARROW, CAP, 3), 1, 2).reshape(SLOTS, 3)
    return (profile, tracer_offsets, tracer_cells)
```

```python
import jax
import jax.numpy as jnp
from jax import lax
from jax.experimental import pallas as pl
from jax.experimental.pallas import tpu as pltpu
from jax.sharding import PartitionSpec as P

CAP = 4
HALO = 3
NODES = 6
TIME_INCREMENT = 0.25
SLOT = 16
GROUP = 4


LY1, LZ1, RX1, LY2, LZ2, RX2, SHX, SHY, SHZ, PEER, LIVE, RANK = range(12)


def lagrange_rows(t):
    d = [t - float(m) for m in range(NODES)]
    head = [None, d[0]]
    for m in range(1, NODES - 1):
        head.append(head[-1] * d[m])
    tail = [None] * NODES
    tail[NODES - 2] = d[NODES - 1]
    for m in range(NODES - 3, -1, -1):
        tail[m] = tail[m + 1] * d[m + 1]
    out = []
    for i in range(NODES):
        scale = 1.0
        for m in range(NODES):
            if m != i:
                scale *= i - m
        if i == 0:
            product = tail[0]
        elif i == NODES - 1:
            product = head[NODES - 1]
        else:
            product = head[i] * tail[i]
        out.append(product * (1.0 / scale))
    return out


def advance_kernel(
    table, own, low_y, high_y, low_z, high_z, low_corners, high_corners,
    offsets, binning, cell_rows, sent, grid, weights, early, later
):
    comps, rows_y, rows_z, lanes = own.shape
    blocks = offsets.shape[1]
    halves = offsets.shape[2] // lanes
    ext_z = rows_z + 2 * HALO
    step_y = ext_z * 16

    def row_of(y, z):
        return (y * ext_z + z) * 16

    def place_y(source, y_in, y_out):
        for c in range(comps):
            v = pltpu.roll(source[c, y_in], ((y_out & 7) * SLOT), 1)
            grid[pl.ds(row_of(y_out, HALO) + c, rows_z, stride=16), :] = v

    def own_row(y, carry):
        place_y(own, y, y + HALO)
        return carry

    lax.fori_loop(0, rows_y, own_row, 0)
    for y in range(HALO):
        place_y(low_y, y, y)
        place_y(high_y, y, y + HALO + rows_y)

    def place_z(c, carry):
        for source, z_base in ((low_z, 0), (high_z, HALO + rows_z)):
            for z in range(HALO):
                for y in range(0, rows_y, 8):
                    v = pltpu.roll(source[c, z, pl.ds(y, 8), :], 0, 1, stride=SLOT, stride_axis=0)
                    v = pltpu.roll(v, HALO * SLOT, 1)
                    grid[pl.ds(row_of(y + HALO, z_base + z) + c, 8, stride=step_y), :] = v
        return carry

    lax.fori_loop(0, comps, place_z, 0)

    def place_corners(c, carry):
        for source, z_base in ((low_corners, 0), (high_corners, HALO + rows_z)):
            for y in range(2 * HALO):
                y_out = y if y < HALO else y + rows_y
                v = source[c, y]
                if (y_out & 7) * SLOT:
                    v = pltpu.roll(v, (y_out & 7) * SLOT, 1)
                grid[pl.ds(row_of(y_out, z_base) + c, HALO, stride=16), :] = v
        return carry

    lax.fori_loop(0, comps, place_corners, 0)

    zero_rows = jnp.zeros((8, lanes), jnp.float32)

    def store_weights(dim, h, first, t):
        rows = lagrange_rows(t)
        for i in range(NODES):
            weights[dim, h, pl.ds(first * 8 + i, 8, stride=8), :] = rows[i]

    def anchor_of(dim, h, first):
        return 2.0 + offsets[dim, pl.ds(first, 8), pl.ds(h * lanes, lanes)]

    for first in range(0, blocks, 8):
        for h in range(halves):
            for dim in range(3):
                store_weights(dim, h, first, anchor_of(dim, h, first))
            for i in range(NODES, 8):
                weights[0, h, pl.ds(first * 8 + i, 8, stride=8), :] = zero_rows

    lane = lax.broadcasted_iota(jnp.int32, (16, lanes), 1)
    low_half = (lane & (SLOT - 1)) < 8
    zero8 = jnp.zeros((8, halves * lanes), jnp.float32)
    zero_pad = jnp.zeros((lanes - NODES * SLOT, halves * lanes), jnp.bfloat16)

    def section(b, ly, lz, rx, result):
        turn = (lane - rx) & (lanes - 1)
        slot = turn >> 4
        masks = [slot == j for j in range(1, NODES)]
        back = (lanes - rx) & (lanes - 1)
        base = pl.multiple_of(row_of(ly, lz), 16)
        parts = []
        for k in range(NODES):
            v = grid[pl.ds(base + k * 16, 16), :]
            for j in range(1, NODES):
                v = jnp.where(masks[j - 1], grid[pl.ds(base + (j * ext_z + k) * 16, 16), :], v)
            v = pltpu.roll(v, back, 1)
            top = v.astype(jnp.bfloat16)
            rest = v - top.astype(jnp.float32)
            mixed = jnp.where(low_half, v, pltpu.roll(rest, 8, 1)).astype(jnp.bfloat16)
            parts.append(jnp.concatenate([mixed, top], axis=1))
        left = jnp.concatenate(parts, axis=0)

        def row(dim, i):
            return jnp.concatenate(
                [weights[dim, h, pl.ds(b * 8 + i, 1), :] for h in range(halves)], axis=1
            )

        first = pl.multiple_of(b * 8, 8)
        wx = jnp.concatenate([weights[0, h, pl.ds(first, 8), :] for h in range(halves)], axis=1)
        right_top = []
        right_rest = []
        for j in range(NODES):
            w = wx * row(1, j)
            top = w.astype(jnp.bfloat16).astype(jnp.float32)
            rest = w - top
            right_top.append(jnp.concatenate([top, top], axis=0).astype(jnp.bfloat16))
            right_rest.append(jnp.concatenate([rest, zero8], axis=0).astype(jnp.bfloat16))
        right = jnp.concatenate(right_top + [zero_pad] + right_rest + [zero_pad], axis=0)
        planes = jnp.dot(left, right, preferred_element_type=jnp.float32)
        total = planes[0:16] * row(2, 0)
        for k in range(1, NODES):
            total = total + planes[k * 16 : (k + 1) * 16] * row(2, k)
        out = pl.multiple_of(b * 16, 16)
        for h in range(halves):
            result[h, pl.ds(out, 16), :] = total[:, h * lanes : (h + 1) * lanes]

    live = table[LIVE, 0]
    groups = (live + GROUP - 1) // GROUP

    def first_step(g, carry):
        for u in range(GROUP):
            b = g * GROUP + u
            section(b, table[LY1, b], table[LZ1, b], table[RX1, b], early)
        return carry

    lax.fori_loop(0, groups, first_step, 0)

    row8 = lax.broadcasted_iota(jnp.int32, (8, lanes), 0)

    def component(result, c, h, first):
        return result[h, pl.ds(first * 16 + c, 8, stride=16), :]

    for first in range(0, blocks, 8):

        @pl.when(first < live)
        def _():
            for dim in range(3):
                shift = jnp.zeros((8, lanes), jnp.float32)
                for u in range(8):
                    shift = jnp.where(row8 == u, table[SHX + dim, first + u].astype(jnp.float32), shift)
                for h in range(halves):
                    t = anchor_of(dim, h, first) + TIME_INCREMENT * component(early, dim, h, first) + shift
                    store_weights(dim, h, first, t)

    def second_step(g, carry):
        for u in range(GROUP):
            b = g * GROUP + u
            section(b, table[LY2, b], table[LZ2, b], table[RX2, b], later)
        return carry

    lax.fori_loop(0, groups, second_step, 0)

    lane8 = lax.broadcasted_iota(jnp.int32, (8, lanes), 1)

    def invariants(result, first):
        strain = jnp.zeros((8, lanes), jnp.float32)
        rotation = jnp.zeros((8, lanes), jnp.float32)
        for h in range(halves):
            g = [[component(result, 3 + 3 * a + c, h, first) for c in range(3)] for a in range(3)]
            for a in range(3):
                strain = strain + g[a][a] * g[a][a]
                for c in range(a + 1, 3):
                    plus = g[a][c] + g[c][a]
                    minus = g[a][c] - g[c][a]
                    strain = strain + 0.5 * (plus * plus)
                    rotation = rotation + 0.5 * (minus * minus)
        return jnp.sum(strain, axis=1, keepdims=True), jnp.sum(rotation, axis=1, keepdims=True)

    grid[0:8, :] = jnp.zeros((8, lanes), jnp.float32)
    for first in range(0, blocks, 8):

        @pl.when(first < live)
        def _():
            four = invariants(early, first) + invariants(later, first)
            spread = jnp.where(lane8 < 16, four[0], jnp.where(lane8 < 32, four[1], jnp.where(lane8 < 48, four[2], four[3])))
            bins = binning[pl.ds(first, 8), :]
            grid[0:8, :] = grid[0:8, :] + jnp.where(bins > 0, spread, 0.0)

            for dim in range(3):
                for h in range(halves):
                    u = component(early, dim, h, first) + component(later, dim, h, first)
                    weights[dim, h, pl.ds(first, 8), :] = anchor_of(dim, h, first) + (0.5 * TIME_INCREMENT) * u

    statistics = jnp.sum(grid[0:8, :], axis=0, keepdims=True)

    peers, per = sent.shape[0], sent.shape[1]

    def clear(n, carry):
        for r in range(per - 1):
            sent[n, r] = jnp.zeros((1, lanes), jnp.float32)
        sent[n, per - 1] = statistics
        return carry

    lax.fori_loop(0, peers, clear, 0)

    def deliver(b, carry):
        peer = table[PEER, b]
        rank = table[RANK, b]
        for dim in range(3):
            for h in range(halves):
                sent[peer, (dim * halves + h) * CAP + rank] = weights[dim, h, pl.ds(b, 1), :]
        sent[peer, per - 1] = sent[peer, per - 1] + cell_rows[pl.ds(b, 1), :]
        return carry

    lax.fori_loop(0, live, deliver, 0)


def unpack_kernel(received, profile, moved, cells, lines, gathered, *, scale):
    peers, per, _, lanes = received.shape
    halves = moved.shape[2] // lanes

    def take(n, carry):
        for dim in range(3):
            for h in range(halves):
                for r in range(CAP):
                    part = dim * halves + h
                    lines[part, pl.ds(n * CAP + r, 1), :] = received[n, part * CAP + r]
        gathered[pl.ds(n, 1), :] = received[n, per - 1]
        return carry

    lax.fori_loop(0, peers, take, 0)
    for dim in range(3):
        for h in range(halves):
            moved[dim, :, h * lanes : (h + 1) * lanes] = lines[dim * halves + h]
    shared = gathered[...]
    total = jnp.sum(shared, axis=0, keepdims=True) * scale
    for r in range(4):
        profile[r : r + 1, :] = total[:, r * 16 : (r + 1) * 16]
    width = cells.shape[1]
    source = lax.broadcasted_iota(jnp.int32, (lanes, width), 0)
    target = lax.broadcasted_iota(jnp.int32, (lanes, width), 1)
    place = lax.broadcasted_iota(jnp.int32, (peers, width), 1)
    peer = lax.broadcasted_iota(jnp.int32, (peers, width), 0)
    mine = (place >> 2) == peer
    top = shared.astype(jnp.bfloat16)
    rest = (shared - top.astype(jnp.float32)).astype(jnp.bfloat16)
    for dim in range(3):
        choose = (source == 64 + 3 * (target & 3) + dim).astype(jnp.float32).astype(jnp.bfloat16)
        value = jnp.dot(top, choose, preferred_element_type=jnp.float32) + jnp.dot(
            rest, choose, preferred_element_type=jnp.float32
        )
        row = jnp.sum(jnp.where(mine, value, 0.0), axis=0, keepdims=True)
        cells[dim : dim + 1, :] = row.astype(jnp.int32) - 1


def vmem():
    return pl.BlockSpec(memory_space=pltpu.VMEM)


def advance(table, pieces, offsets, binning, cell_rows, peers):
    own = pieces[0]
    comps, rows_y, rows_z, lanes = own.shape
    _, blocks, tracers = offsets.shape
    halves = tracers // lanes
    return pl.pallas_call(
        advance_kernel,
        out_shape=jax.ShapeDtypeStruct((peers, halves * 3 * CAP + 1, 1, lanes), jnp.float32),
        in_specs=[pl.BlockSpec(memory_space=pltpu.SMEM)] + [vmem()] * (len(pieces) + 3),
        out_specs=vmem(),
        scratch_shapes=[
            pltpu.VMEM(((rows_y + 2 * HALO) * (rows_z + 2 * HALO) * 16 + 64, lanes), jnp.float32),
            pltpu.VMEM((3, halves, blocks * 8 + 8, lanes), jnp.float32),
            pltpu.VMEM((halves, blocks * 16 + 16, lanes), jnp.float32),
            pltpu.VMEM((halves, blocks * 16 + 16, lanes), jnp.float32),
        ],
        compiler_params=pltpu.CompilerParams(vmem_limit_bytes=40 * 1024 * 1024),
        name="advance",
    )(table, *pieces, offsets, binning, cell_rows)


def unpack(received, peers, rows_y, tracers):
    return pl.pallas_call(
        lambda *refs: unpack_kernel(*refs, scale=1.0 / (tracers * peers)),
        out_shape=(
            jax.ShapeDtypeStruct((4, rows_y), jnp.float32),
            jax.ShapeDtypeStruct((3, peers * CAP, tracers), jnp.float32),
            jax.ShapeDtypeStruct((3, peers * CAP), jnp.int32),
        ),
        in_specs=[vmem()],
        out_specs=(vmem(), vmem(), vmem()),
        scratch_shapes=[
            pltpu.VMEM((3 * tracers // received.shape[3], peers * CAP, received.shape[3]), jnp.float32),
            pltpu.VMEM((peers, received.shape[3]), jnp.float32),
        ],
        name="unpack",
    )(received)


def neighbour(x, axis, step):
    count = lax.axis_size(axis)
    return lax.ppermute(x, axis, [(i, (i + step) % count) for i in range(count)])


def halo(flow_field):
    rows_y, rows_z = flow_field.shape[1:3]
    by_z = jnp.swapaxes(flow_field, 1, 2)
    low_y = neighbour(flow_field[:, rows_y - HALO :], "wide", 1)
    high_y = neighbour(flow_field[:, :HALO], "wide", -1)
    low_z = neighbour(by_z[:, rows_z - HALO :], "narrow", 1)
    high_z = neighbour(by_z[:, :HALO], "narrow", -1)
    both_y = jnp.concatenate([low_y, high_y], axis=1)
    low_corners = neighbour(both_y[:, :, rows_z - HALO :], "narrow", 1)
    high_corners = neighbour(both_y[:, :, :HALO], "narrow", -1)
    return (flow_field, low_y, high_y, low_z, high_z, low_corners, high_corners)


def plan(cells_first, cells_second, live_counts, destination, extents, first_y, first_z, lanes):
    blocks = cells_first.shape[1]
    index = jnp.arange(blocks, dtype=jnp.int32)

    def tile(cells):
        ly = (cells[1] - first_y + HALO) % extents[1]
        lz = (cells[2] - first_z + HALO) % extents[2]
        return [ly, lz, (cells[0] + SLOT * (ly & 7)) & (lanes - 1)]

    shift = [
        (cells_first[d] - cells_second[d] + extents[d] // 2) % extents[d] - extents[d] // 2 for d in range(3)
    ]
    target = destination[0]
    same = (target[:, None] == target[None, :]) & (index[None, :] < index[:, None])
    rank = jnp.sum(same.astype(jnp.int32), axis=1)
    table = jnp.stack(
        tile(cells_first)
        + tile(cells_second)
        + shift
        + [target, jnp.broadcast_to(live_counts, (blocks,)), rank]
    )
    lane = jnp.arange(lanes, dtype=jnp.int32)[None, :]
    column = (cells_first[1] + 2 - first_y) % extents[1]
    alive = index[:, None] < live_counts
    binning = jnp.where(alive & (lane < 64) & ((lane & 15) == column[:, None]), 1.0, 0.0)
    place = lane - 64 - 3 * rank[:, None]
    cell = jnp.where(place == 0, cells_first[0][:, None], jnp.where(place == 1, cells_first[1][:, None], cells_first[2][:, None]))
    cell_rows = jnp.where((place >= 0) & (place < 3), (cell + 1).astype(jnp.float32), 0.0)
    return table, binning, cell_rows


def local(flow_field, offsets, cells_first, cells_second, live_counts, destination):
    wide_count = lax.axis_size("wide")
    narrow_count = lax.axis_size("narrow")
    _, rows_y, rows_z, rows_x = flow_field.shape
    tracers = offsets.shape[2]
    pieces = halo(flow_field)
    table, binning, cell_rows = plan(
        cells_first.T, cells_second.T, live_counts, destination.T,
        (rows_x, rows_y * wide_count, rows_z * narrow_count),
        lax.axis_index("wide") * rows_y, lax.axis_index("narrow") * rows_z, rows_x,
    )
    sent = advance(table, pieces, jnp.swapaxes(offsets, 0, 1), binning, cell_rows, narrow_count)
    received = lax.all_to_all(sent, "narrow", split_axis=0, concat_axis=0, tiled=True)
    profile, moved, cells = unpack(received, narrow_count, rows_y, tracers)
    return profile, jnp.swapaxes(moved, 0, 1), cells.T


def solution(mesh):
    return jax.shard_map(
        local,
        mesh=mesh,
        in_specs=(
            P(None, "wide", "narrow", None),
            P(("wide", "narrow"), None, None),
            P(("wide", "narrow"), None),
            P(("wide", "narrow"), None),
            P(("wide", "narrow")),
            P(("wide", "narrow"), None),
        ),
        out_specs=(P(None, "wide"), P(("wide", "narrow"), None, None), P(("wide", "narrow"), None)),
        check_vma=False,
    )
```

```python
import jax
import jax.numpy as jnp
from jax import lax
from jax.experimental import pallas as pl
from jax.experimental.pallas import tpu as pltpu
from jax.sharding import PartitionSpec as P

CAP = 4
HALO = 3
NODES = 6
EXT_Z = 14
TIME_INCREMENT = 0.25
SLOT = 16
GROUP = 16


LY1, LZ1, RX1, LY2, LZ2, RX2, PEER, LIVE, RANK = range(9)


def lagrange_rows(t):
    d = [t - float(m) for m in range(NODES)]
    head = [None, d[0]]
    for m in range(1, NODES - 1):
        head.append(head[-1] * d[m])
    tail = [None] * NODES
    tail[NODES - 2] = d[NODES - 1]
    for m in range(NODES - 3, -1, -1):
        tail[m] = tail[m + 1] * d[m + 1]
    out = []
    for i in range(NODES):
        scale = 1.0
        for m in range(NODES):
            if m != i:
                scale *= i - m
        if i == 0:
            product = tail[0]
        elif i == NODES - 1:
            product = head[NODES - 1]
        else:
            product = head[i] * tail[i]
        out.append(product * (1.0 / scale))
    return out


def row_of(y, z, ext_z):
    return (y * ext_z + z) * 16


def store_weights(weights, dim, h, first, t):
    rows = lagrange_rows(t)
    for i in range(NODES):
        weights[dim, h, pl.ds(first * 8 + i, 8, stride=8), :] = rows[i]


def anchor_of(offsets, dim, h, first, lanes):
    return 2.0 + offsets[dim, pl.ds(first, 8), pl.ds(h * lanes, lanes)]


def prepare_kernel(own, low_y, high_y, low_z, high_z, offsets, grid, weights, sent):
    comps, rows_y, rows_z, lanes = own.shape
    blocks = offsets.shape[1]
    halves = offsets.shape[2] // lanes
    ext_z = rows_z + 2 * HALO

    def place_y(source, y_in, y_out):
        for c in range(comps):
            v = pltpu.roll(source[c, y_in], ((y_out & 7) * SLOT), 1)
            grid[pl.ds(row_of(y_out, HALO, ext_z) + c, rows_z, stride=16), :] = v

    def own_row(y, carry):
        place_y(own, y, y + HALO)
        return carry

    lax.fori_loop(0, rows_y, own_row, 0)
    for y in range(HALO):
        place_y(low_y, y, y)
        place_y(high_y, y, y + HALO + rows_y)

    def place_z(c, carry):
        for source, z_base in ((low_z, 0), (high_z, HALO + rows_z)):
            for z in range(HALO):
                for y in range(0, rows_y, 8):
                    v = pltpu.roll(source[c, z, pl.ds(y, 8), :], 0, 1, stride=SLOT, stride_axis=0)
                    v = pltpu.roll(v, HALO * SLOT, 1)
                    grid[pl.ds(row_of(y + HALO, z_base + z, ext_z) + c, 8, stride=ext_z * 16), :] = v
        return carry

    lax.fori_loop(0, comps, place_z, 0)

    zero_rows = jnp.zeros((8, lanes), jnp.float32)
    for first in range(0, blocks, 8):
        for h in range(halves):
            for dim in range(3):
                store_weights(weights, dim, h, first, anchor_of(offsets, dim, h, first, lanes))
            for i in range(NODES, 8):
                weights[0, h, pl.ds(first * 8 + i, 8, stride=8), :] = zero_rows

    def clear(n, carry):
        for r in range(sent.shape[1]):
            sent[n, r] = jnp.zeros((1, lanes), jnp.float32)
        return carry

    lax.fori_loop(0, sent.shape[0], clear, 0)


def advance_kernel(
    table, low_corners, high_corners, offsets, traits, cell_rows, grid_in, weights_in, sent_in,
    grid, weights, sent, early, later
):
    comps, rows_c, _, lanes = low_corners.shape
    blocks = offsets.shape[1]
    halves = offsets.shape[2] // lanes
    ext_z = EXT_Z
    rows_y = (grid.shape[0] - 64) // (ext_z * 16) - rows_c
    rows_z = ext_z - 2 * HALO

    def place_corners(c, carry):
        for source, z_base in ((low_corners, 0), (high_corners, HALO + rows_z)):
            for y in range(2 * HALO):
                y_out = y if y < HALO else y + rows_y
                v = source[c, y]
                if (y_out & 7) * SLOT:
                    v = pltpu.roll(v, (y_out & 7) * SLOT, 1)
                grid[pl.ds(row_of(y_out, z_base, ext_z) + c, HALO, stride=16), :] = v
        return carry

    lax.fori_loop(0, comps, place_corners, 0)

    lane = lax.broadcasted_iota(jnp.int32, (16, lanes), 1)
    low_half = (lane & (SLOT - 1)) < 8
    zero8 = jnp.zeros((8, halves * lanes), jnp.float32)
    zero_pad = jnp.zeros((lanes - NODES * SLOT, halves * lanes), jnp.bfloat16)

    def section(b, ly, lz, rx, result):
        turn = (lane - rx) & (lanes - 1)
        slot = turn >> 4
        masks = [slot == j for j in range(1, NODES)]
        back = (lanes - rx) & (lanes - 1)
        base = pl.multiple_of(row_of(ly, lz, ext_z), 16)
        parts = []
        for k in range(NODES):
            v = grid[pl.ds(base + k * 16, 16), :]
            for j in range(1, NODES):
                v = jnp.where(masks[j - 1], grid[pl.ds(base + (j * ext_z + k) * 16, 16), :], v)
            v = pltpu.roll(v, back, 1)
            top = v.astype(jnp.bfloat16)
            rest = v - top.astype(jnp.float32)
            mixed = jnp.where(low_half, v, pltpu.roll(rest, 8, 1)).astype(jnp.bfloat16)
            parts.append(jnp.concatenate([mixed, top], axis=1))
        left = jnp.concatenate(parts, axis=0)

        def row(dim, i):
            return jnp.concatenate(
                [weights[dim, h, pl.ds(b * 8 + i, 1), :] for h in range(halves)], axis=1
            )

        first = pl.multiple_of(b * 8, 8)
        wx = jnp.concatenate([weights[0, h, pl.ds(first, 8), :] for h in range(halves)], axis=1)
        right_top = []
        right_rest = []
        for j in range(NODES):
            w = wx * row(1, j)
            top = w.astype(jnp.bfloat16).astype(jnp.float32)
            rest = w - top
            right_top.append(jnp.concatenate([top, top], axis=0).astype(jnp.bfloat16))
            right_rest.append(jnp.concatenate([rest, zero8], axis=0).astype(jnp.bfloat16))
        right = jnp.concatenate(right_top + [zero_pad] + right_rest + [zero_pad], axis=0)
        planes = jnp.dot(left, right, preferred_element_type=jnp.float32)
        total = planes[0:16] * row(2, 0)
        for k in range(1, NODES):
            total = total + planes[k * 16 : (k + 1) * 16] * row(2, k)
        out = pl.multiple_of(b * 16, 16)
        for h in range(halves):
            result[h, pl.ds(out, 16), :] = total[:, h * lanes : (h + 1) * lanes]

    live = table[LIVE, 0]
    groups = (live + GROUP - 1) // GROUP

    def first_step(g, carry):
        for u in range(GROUP):
            b = g * GROUP + u
            section(b, table[LY1, b], table[LZ1, b], table[RX1, b], early)
        return carry

    lax.fori_loop(0, groups, first_step, 0)

    def component(result, c, h, first):
        return result[h, pl.ds(first * 16 + c, 8, stride=16), :]

    for first in range(0, blocks, 8):

        @pl.when(first < live)
        def _():
            for dim in range(3):
                shift = jnp.broadcast_to(traits[pl.ds(first, 8), 64 + dim : 65 + dim], (8, lanes))
                for h in range(halves):
                    t = anchor_of(offsets, dim, h, first, lanes) + TIME_INCREMENT * component(early, dim, h, first) + shift
                    store_weights(weights, dim, h, first, t)

    def second_step(g, carry):
        for u in range(GROUP):
            b = g * GROUP + u
            section(b, table[LY2, b], table[LZ2, b], table[RX2, b], later)
        return carry

    lax.fori_loop(0, groups, second_step, 0)

    lane8 = lax.broadcasted_iota(jnp.int32, (8, lanes), 1)

    def invariants(result, first):
        strain = jnp.zeros((8, lanes), jnp.float32)
        rotation = jnp.zeros((8, lanes), jnp.float32)
        for h in range(halves):
            g = [[component(result, 3 + 3 * a + c, h, first) for c in range(3)] for a in range(3)]
            for a in range(3):
                strain = strain + g[a][a] * g[a][a]
                for c in range(a + 1, 3):
                    plus = g[a][c] + g[c][a]
                    minus = g[a][c] - g[c][a]
                    strain = strain + 0.5 * (plus * plus)
                    rotation = rotation + 0.5 * (minus * minus)
        return jnp.sum(strain, axis=1, keepdims=True), jnp.sum(rotation, axis=1, keepdims=True)

    grid[0:8, :] = jnp.zeros((8, lanes), jnp.float32)
    for first in range(0, blocks, 8):

        @pl.when(first < live)
        def _():
            four = invariants(early, first) + invariants(later, first)
            spread = jnp.where(lane8 < 16, four[0], jnp.where(lane8 < 32, four[1], jnp.where(lane8 < 48, four[2], four[3])))
            bins = (traits[pl.ds(first, 8), :] > 0) & (lane8 < 64)
            grid[0:8, :] = grid[0:8, :] + jnp.where(bins, spread, 0.0)

            for dim in range(3):
                for h in range(halves):
                    u = component(early, dim, h, first) + component(later, dim, h, first)
                    weights[dim, h, pl.ds(first, 8), :] = anchor_of(offsets, dim, h, first, lanes) + (0.5 * TIME_INCREMENT) * u

    statistics = jnp.sum(grid[0:8, :], axis=0, keepdims=True)

    peers, per = sent.shape[0], sent.shape[1]

    def share(n, carry):
        sent[n, per - 1] = statistics
        return carry

    lax.fori_loop(0, peers, share, 0, unroll=8)

    def deliver(b, carry):
        peer = table[PEER, b]
        rank = table[RANK, b]
        for dim in range(3):
            for h in range(halves):
                sent[peer, (dim * halves + h) * CAP + rank] = weights[dim, h, pl.ds(b, 1), :]
        sent[peer, per - 1] = sent[peer, per - 1] + cell_rows[pl.ds(b, 1), :]
        return carry

    lax.fori_loop(0, live, deliver, 0)


def unpack_kernel(received, profile, moved, cells, lines, gathered, *, scale):
    peers, per, _, lanes = received.shape
    halves = moved.shape[2] // lanes

    def take(n, carry):
        for dim in range(3):
            for h in range(halves):
                for r in range(CAP):
                    part = dim * halves + h
                    lines[part, pl.ds(n * CAP + r, 1), :] = received[n, part * CAP + r]
        gathered[pl.ds(n, 1), :] = received[n, per - 1]
        return carry

    lax.fori_loop(0, peers, take, 0)
    for dim in range(3):
        for h in range(halves):
            moved[dim, :, h * lanes : (h + 1) * lanes] = lines[dim * halves + h]
    shared = gathered[...]
    total = jnp.sum(shared, axis=0, keepdims=True) * scale
    for r in range(4):
        profile[r : r + 1, :] = total[:, r * 16 : (r + 1) * 16]
    width = cells.shape[1]
    source = lax.broadcasted_iota(jnp.int32, (lanes, width), 0)
    target = lax.broadcasted_iota(jnp.int32, (lanes, width), 1)
    place = lax.broadcasted_iota(jnp.int32, (peers, width), 1)
    peer = lax.broadcasted_iota(jnp.int32, (peers, width), 0)
    mine = (place >> 2) == peer
    top = shared.astype(jnp.bfloat16)
    rest = (shared - top.astype(jnp.float32)).astype(jnp.bfloat16)
    for dim in range(3):
        choose = (source == 64 + 3 * (target & 3) + dim).astype(jnp.float32).astype(jnp.bfloat16)
        value = jnp.dot(top, choose, preferred_element_type=jnp.float32) + jnp.dot(
            rest, choose, preferred_element_type=jnp.float32
        )
        row = jnp.sum(jnp.where(mine, value, 0.0), axis=0, keepdims=True)
        cells[dim : dim + 1, :] = row.astype(jnp.int32) - 1


def vmem():
    return pl.BlockSpec(memory_space=pltpu.VMEM)


def prepare(own, low_y, high_y, low_z, high_z, offsets, peers):
    _, rows_y, rows_z, lanes = own.shape
    _, blocks, tracers = offsets.shape
    halves = tracers // lanes
    return pl.pallas_call(
        prepare_kernel,
        out_shape=(
            jax.ShapeDtypeStruct(((rows_y + 2 * HALO) * (rows_z + 2 * HALO) * 16 + 64, lanes), jnp.float32),
            jax.ShapeDtypeStruct((3, halves, blocks * 8 + 8, lanes), jnp.float32),
            jax.ShapeDtypeStruct((peers, halves * 3 * CAP + 1, 1, lanes), jnp.float32),
        ),
        in_specs=[vmem()] * 6,
        out_specs=(vmem(), vmem(), vmem()),
        compiler_params=pltpu.CompilerParams(vmem_limit_bytes=40 * 1024 * 1024),
        cost_estimate=pl.CostEstimate(flops=30_000_000, bytes_accessed=8_000_000, transcendentals=0),
        name="prepare",
    )(own, low_y, high_y, low_z, high_z, offsets)


def advance(table, corners, offsets, traits, cell_rows, prepared):
    lanes = corners[0].shape[-1]
    _, blocks, tracers = offsets.shape
    halves = tracers // lanes
    return pl.pallas_call(
        advance_kernel,
        out_shape=tuple(jax.ShapeDtypeStruct(x.shape, x.dtype) for x in prepared),
        in_specs=[pl.BlockSpec(memory_space=pltpu.SMEM)] + [vmem()] * 8,
        out_specs=(vmem(), vmem(), vmem()),
        input_output_aliases={6: 0, 7: 1, 8: 2},
        scratch_shapes=[
            pltpu.VMEM((halves, blocks * 16 + 16, lanes), jnp.float32),
            pltpu.VMEM((halves, blocks * 16 + 16, lanes), jnp.float32),
        ],
        compiler_params=pltpu.CompilerParams(vmem_limit_bytes=40 * 1024 * 1024),
        name="advance",
    )(table, *corners, offsets, traits, cell_rows, *prepared)[2]


def unpack(received, peers, rows_y, tracers):
    return pl.pallas_call(
        lambda *refs: unpack_kernel(*refs, scale=1.0 / (tracers * peers)),
        out_shape=(
            jax.ShapeDtypeStruct((4, rows_y), jnp.float32),
            jax.ShapeDtypeStruct((3, peers * CAP, tracers), jnp.float32),
            jax.ShapeDtypeStruct((3, peers * CAP), jnp.int32),
        ),
        in_specs=[vmem()],
        out_specs=(vmem(), vmem(), vmem()),
        scratch_shapes=[
            pltpu.VMEM((3 * tracers // received.shape[3], peers * CAP, received.shape[3]), jnp.float32),
            pltpu.VMEM((peers, received.shape[3]), jnp.float32),
        ],
        name="unpack",
    )(received)


def neighbour(x, axis, step, name):
    count = lax.axis_size(axis)
    with jax.named_scope(name):
        return lax.ppermute(x, axis, [(i, (i + step) % count) for i in range(count)])


def halo(flow_field):
    rows_y, rows_z = flow_field.shape[1:3]
    by_z = jnp.swapaxes(flow_field, 1, 2)
    low_y = neighbour(flow_field[:, rows_y - HALO :], "wide", 1, "low_y")
    high_y = neighbour(flow_field[:, :HALO], "wide", -1, "high_y")
    low_z = neighbour(by_z[:, rows_z - HALO :], "narrow", 1, "low_z")
    high_z = neighbour(by_z[:, :HALO], "narrow", -1, "high_z")

    def corners(start):
        return jnp.concatenate([low_y[:, :, start : start + HALO], high_y[:, :, start : start + HALO]], axis=1)

    low_corners = neighbour(corners(rows_z - HALO), "narrow", 1, "low_corners")
    high_corners = neighbour(corners(0), "narrow", -1, "high_corners")
    return (flow_field, low_y, high_y, low_z, high_z), (low_corners, high_corners)


def plan(cells_first, cells_second, live_counts, destination, extents, first_y, first_z, lanes):
    blocks = cells_first.shape[1]
    index = jnp.arange(blocks, dtype=jnp.int32)

    def tile(cells):
        ly = (cells[1] - first_y + HALO) % extents[1]
        lz = (cells[2] - first_z + HALO) % extents[2]
        return [ly, lz, (cells[0] + SLOT * (ly & 7)) & (lanes - 1)]

    shift = [
        (cells_first[d] - cells_second[d] + extents[d] // 2) % extents[d] - extents[d] // 2 for d in range(3)
    ]
    target = destination[0]
    same = (target[:, None] == target[None, :]) & (index[None, :] < index[:, None])
    rank = jnp.sum(same.astype(jnp.int32), axis=1)
    table = jnp.stack(
        tile(cells_first)
        + tile(cells_second)
        + [target, jnp.broadcast_to(live_counts, (blocks,)), rank]
    )
    lane = jnp.arange(lanes, dtype=jnp.int32)[None, :]
    column = (cells_first[1] + 2 - first_y) % extents[1]
    alive = index[:, None] < live_counts
    traits = jnp.where(alive & (lane < 64) & ((lane & 15) == column[:, None]), 1.0, 0.0)
    for d in range(3):
        traits = jnp.where(lane == 64 + d, shift[d].astype(jnp.float32)[:, None], traits)
    place = lane - 64 - 3 * rank[:, None]
    cell = jnp.where(place == 0, cells_first[0][:, None], jnp.where(place == 1, cells_first[1][:, None], cells_first[2][:, None]))
    cell_rows = jnp.where((place >= 0) & (place < 3), (cell + 1).astype(jnp.float32), 0.0)
    return table, traits, cell_rows


def local(flow_field, offsets, cells_first, cells_second, live_counts, destination):
    wide_count = lax.axis_size("wide")
    narrow_count = lax.axis_size("narrow")
    _, rows_y, rows_z, rows_x = flow_field.shape
    tracers = offsets.shape[2]
    assert rows_z + 2 * HALO == EXT_Z
    pieces, corners = halo(flow_field)
    offsets = jnp.swapaxes(offsets, 0, 1)
    prepared = prepare(*pieces, offsets, narrow_count)
    table, traits, cell_rows = plan(
        cells_first.T, cells_second.T, live_counts, destination.T,
        (rows_x, rows_y * wide_count, rows_z * narrow_count),
        lax.axis_index("wide") * rows_y, lax.axis_index("narrow") * rows_z, rows_x,
    )
    sent = advance(table, corners, offsets, traits, cell_rows, prepared)
    received = lax.all_to_all(sent, "narrow", split_axis=0, concat_axis=0, tiled=True)
    profile, moved, cells = unpack(received, narrow_count, rows_y, tracers)
    return profile, jnp.swapaxes(moved, 0, 1), cells.T


def solution(mesh):
    return jax.shard_map(
        local,
        mesh=mesh,
        in_specs=(
            P(None, "wide", "narrow", None),
            P(("wide", "narrow"), None, None),
            P(("wide", "narrow"), None),
            P(("wide", "narrow"), None),
            P(("wide", "narrow")),
            P(("wide", "narrow"), None),
        ),
        out_specs=(P(None, "wide"), P(("wide", "narrow"), None, None), P(("wide", "narrow"), None)),
        check_vma=False,
    )
```

```python
import jax
import jax.numpy as jnp
from jax import lax
from jax.experimental import pallas as pl
from jax.experimental.pallas import tpu as pltpu
from jax.sharding import PartitionSpec as P

CAP = 4
HALO = 3
NODES = 6
EXT_Z = 14
TIME_INCREMENT = 0.25
SLOT = 16
UNPACK_STEPS = 2
GROUP = 16


LY1, LZ1, RX1, LY2, LZ2, RX2, PEER, RANK = range(8)


def lagrange_rows(t):
    d = [t - float(m) for m in range(NODES)]
    head = [None, d[0]]
    for m in range(1, NODES - 1):
        head.append(head[-1] * d[m])
    tail = [None] * NODES
    tail[NODES - 2] = d[NODES - 1]
    for m in range(NODES - 3, -1, -1):
        tail[m] = tail[m + 1] * d[m + 1]
    out = []
    for i in range(NODES):
        scale = 1.0
        for m in range(NODES):
            if m != i:
                scale *= i - m
        if i == 0:
            product = tail[0]
        elif i == NODES - 1:
            product = head[NODES - 1]
        else:
            product = head[i] * tail[i]
        out.append(product * (1.0 / scale))
    return out


def row_of(y, z, ext_z):
    return (y * ext_z + z) * 16


def store_weights(weights, dim, h, first, t):
    rows = lagrange_rows(t)
    for i in range(NODES):
        weights[dim, h, pl.ds(first * 8 + i, 8, stride=8), :] = rows[i]


def anchor_of(offsets, dim, h, first, lanes):
    return 2.0 + offsets[dim, pl.ds(first, 8), pl.ds(h * lanes, lanes)]


def prepare_kernel(own, low_y, high_y, low_z, high_z, offsets, grid, weights, sent):
    comps, rows_y, rows_z, lanes = own.shape
    blocks = offsets.shape[1]
    halves = offsets.shape[2] // lanes
    ext_z = rows_z + 2 * HALO

    def place_y(source, y_in, y_out):
        for c in range(comps):
            v = pltpu.roll(source[c, y_in], ((y_out & 7) * SLOT), 1)
            grid[pl.ds(row_of(y_out, HALO, ext_z) + c, rows_z, stride=16), :] = v

    def own_row(y, carry):
        place_y(own, y, y + HALO)
        return carry

    lax.fori_loop(0, rows_y, own_row, 0, unroll=4)
    for y in range(HALO):
        place_y(low_y, y, y)
        place_y(high_y, y, y + HALO + rows_y)

    def place_z(c, carry):
        for source, z_base in ((low_z, 0), (high_z, HALO + rows_z)):
            for z in range(HALO):
                for y in range(0, rows_y, 8):
                    v = pltpu.roll(source[c, z, pl.ds(y, 8), :], 0, 1, stride=SLOT, stride_axis=0)
                    v = pltpu.roll(v, HALO * SLOT, 1)
                    grid[pl.ds(row_of(y + HALO, z_base + z, ext_z) + c, 8, stride=ext_z * 16), :] = v
        return carry

    lax.fori_loop(0, comps, place_z, 0, unroll=4)

    zero_rows = jnp.zeros((8, lanes), jnp.float32)
    for first in range(0, blocks, 8):
        for h in range(halves):
            for dim in range(3):
                store_weights(weights, dim, h, first, anchor_of(offsets, dim, h, first, lanes))
            for i in range(NODES, 8):
                weights[0, h, pl.ds(first * 8 + i, 8, stride=8), :] = zero_rows

    def clear(n, carry):
        for r in range(sent.shape[1]):
            sent[n, r] = jnp.zeros((1, lanes), jnp.float32)
        return carry

    lax.fori_loop(0, sent.shape[0], clear, 0, unroll=4)


def advance_kernel(
    live_ref, table_in, low_corners, high_corners, offsets, traits, cell_rows, grid_in, weights_in, sent_in,
    grid, weights, sent, early, later, table, table_sem
):
    lanes = low_corners.shape[2]
    comps = low_corners.shape[1] // (2 * HALO)
    pad = jnp.zeros((8 - 2 * HALO, lanes), jnp.float32)
    blocks = offsets.shape[1]
    halves = offsets.shape[2] // lanes
    ext_z = EXT_Z
    rows_y = (grid.shape[0] - 64) // (ext_z * 16) - 2 * HALO
    rows_z = ext_z - 2 * HALO

    fetch = pltpu.make_async_copy(table_in, table, table_sem)
    fetch.start()

    for source, z_base in ((low_corners, 0), (high_corners, HALO + rows_z)):
        for z in range(HALO):
            for c in range(comps):
                v = jnp.concatenate([source[z, pl.ds(c * 2 * HALO, 2 * HALO), :], pad], axis=0)
                v = pltpu.roll(v, 0, 1, stride=SLOT, stride_axis=0)
                low = row_of(0, z_base + z, ext_z) + c
                high = row_of(HALO + rows_y, z_base + z, ext_z) + c
                grid[pl.ds(low, HALO, stride=ext_z * 16), :] = v[:HALO]
                grid[pl.ds(high, HALO, stride=ext_z * 16), :] = v[HALO : 2 * HALO]
    fetch.wait()

    lane = lax.broadcasted_iota(jnp.int32, (16, lanes), 1)
    low_half = (lane & (SLOT - 1)) < 8
    zero8 = jnp.zeros((8, halves * lanes), jnp.float32)
    zero_pad = jnp.zeros((lanes - NODES * SLOT, halves * lanes), jnp.bfloat16)

    def section(b, ly, lz, rx, result):
        turn = (lane - rx) & (lanes - 1)
        slot = turn >> 4
        masks = [slot == j for j in range(1, NODES)]
        back = (lanes - rx) & (lanes - 1)
        base = pl.multiple_of(row_of(ly, lz, ext_z), 16)
        parts = []
        for k in range(NODES):
            v = grid[pl.ds(base + k * 16, 16), :]
            for j in range(1, NODES):
                v = jnp.where(masks[j - 1], grid[pl.ds(base + (j * ext_z + k) * 16, 16), :], v)
            v = pltpu.roll(v, back, 1)
            top = v.astype(jnp.bfloat16)
            rest = v - top.astype(jnp.float32)
            mixed = jnp.where(low_half, v, pltpu.roll(rest, 8, 1)).astype(jnp.bfloat16)
            parts.append(jnp.concatenate([mixed, top], axis=1))
        left = jnp.concatenate(parts, axis=0)

        def row(dim, i):
            return jnp.concatenate(
                [weights[dim, h, pl.ds(b * 8 + i, 1), :] for h in range(halves)], axis=1
            )

        first = pl.multiple_of(b * 8, 8)
        wx = jnp.concatenate([weights[0, h, pl.ds(first, 8), :] for h in range(halves)], axis=1)
        right_top = []
        right_rest = []
        for j in range(NODES):
            w = wx * row(1, j)
            top = w.astype(jnp.bfloat16).astype(jnp.float32)
            rest = w - top
            right_top.append(jnp.concatenate([top, top], axis=0).astype(jnp.bfloat16))
            right_rest.append(jnp.concatenate([rest, zero8], axis=0).astype(jnp.bfloat16))
        right = jnp.concatenate(right_top + [zero_pad] + right_rest + [zero_pad], axis=0)
        planes = jnp.dot(left, right, preferred_element_type=jnp.float32)
        total = planes[0:16] * row(2, 0)
        for k in range(1, NODES):
            total = total + planes[k * 16 : (k + 1) * 16] * row(2, k)
        out = pl.multiple_of(b * 16, 16)
        for h in range(halves):
            result[h, pl.ds(out, 16), :] = total[:, h * lanes : (h + 1) * lanes]

    live = live_ref[0]
    groups = (live + GROUP - 1) // GROUP

    def first_step(g, carry):
        for u in range(GROUP):
            b = g * GROUP + u
            section(b, table[LY1, b], table[LZ1, b], table[RX1, b], early)
        return carry

    lax.fori_loop(0, groups, first_step, 0)

    def component(result, c, h, first):
        return result[h, pl.ds(first * 16 + c, 8, stride=16), :]

    for first in range(0, blocks, 8):

        @pl.when(first < live)
        def _():
            for dim in range(3):
                shift = jnp.broadcast_to(traits[pl.ds(first, 8), 64 + dim : 65 + dim], (8, lanes))
                for h in range(halves):
                    t = anchor_of(offsets, dim, h, first, lanes) + TIME_INCREMENT * component(early, dim, h, first) + shift
                    store_weights(weights, dim, h, first, t)

    def second_step(g, carry):
        for u in range(GROUP):
            b = g * GROUP + u
            section(b, table[LY2, b], table[LZ2, b], table[RX2, b], later)
        return carry

    lax.fori_loop(0, groups, second_step, 0)

    lane8 = lax.broadcasted_iota(jnp.int32, (8, lanes), 1)
    row8 = lax.broadcasted_iota(jnp.int32, (8, lanes), 0)

    def invariants(result, first):
        strain = jnp.zeros((8, lanes), jnp.float32)
        rotation = jnp.zeros((8, lanes), jnp.float32)
        for h in range(halves):
            g = [[component(result, 3 + 3 * a + c, h, first) for c in range(3)] for a in range(3)]
            for a in range(3):
                strain = strain + g[a][a] * g[a][a]
                for c in range(a + 1, 3):
                    plus = g[a][c] + g[c][a]
                    minus = g[a][c] - g[c][a]
                    strain = strain + 0.5 * (plus * plus)
                    rotation = rotation + 0.5 * (minus * minus)
        return jnp.sum(strain, axis=1, keepdims=True), jnp.sum(rotation, axis=1, keepdims=True)

    grid[0:8, :] = jnp.zeros((8, lanes), jnp.float32)
    for first in range(0, blocks, 8):

        @pl.when(first < live)
        def _():
            four = invariants(early, first) + invariants(later, first)
            spread = jnp.where(lane8 < 16, four[0], jnp.where(lane8 < 32, four[1], jnp.where(lane8 < 48, four[2], four[3])))
            bins = (traits[pl.ds(first, 8), :] > 0) & (lane8 < 64) & (row8 + first < live)
            grid[0:8, :] = grid[0:8, :] + jnp.where(bins, spread, 0.0)

            for dim in range(3):
                for h in range(halves):
                    u = component(early, dim, h, first) + component(later, dim, h, first)
                    weights[dim, h, pl.ds(first, 8), :] = anchor_of(offsets, dim, h, first, lanes) + (0.5 * TIME_INCREMENT) * u

    statistics = jnp.sum(grid[0:8, :], axis=0, keepdims=True)

    peers, per = sent.shape[0], sent.shape[1]

    def share(n, carry):
        sent[n, per - 1] = statistics
        return carry

    lax.fori_loop(0, peers, share, 0, unroll=8)

    def deliver(b, carry):
        peer = table[PEER, b]
        rank = table[RANK, b]
        for dim in range(3):
            for h in range(halves):
                sent[peer, (dim * halves + h) * CAP + rank] = weights[dim, h, pl.ds(b, 1), :]
        sent[peer, per - 1] = sent[peer, per - 1] + cell_rows[pl.ds(b, 1), :]
        return carry

    lax.fori_loop(0, live, deliver, 0)


def unpack_kernel(received, profile, moved, cells, lines, gathered, *, scale):
    peers, per, _, lanes = received.shape
    halves = moved.shape[2] // lanes

    def take(n, carry):
        for part in range(3 * halves):
            for r in range(CAP):
                lines[part, pl.ds(n * CAP + r, 1), :] = received[n, part * CAP + r]
        gathered[pl.ds(n, 1), :] = received[n, per - 1]
        return carry

    lax.fori_loop(0, peers, take, 0, unroll=8)
    for dim in range(3):
        for h in range(halves):
            moved[dim, :, h * lanes : (h + 1) * lanes] = lines[dim * halves + h]
    shared = gathered[...]
    total = jnp.sum(shared, axis=0, keepdims=True) * scale
    first_step = pl.program_id(0) == 0
    for r in range(4):
        part = total[:, r * 16 : (r + 1) * 16]
        profile[r : r + 1, :] = part + jnp.where(first_step, 0.0, profile[r : r + 1, :])
    width = cells.shape[1]
    source = lax.broadcasted_iota(jnp.int32, (lanes, width), 0)
    target = lax.broadcasted_iota(jnp.int32, (lanes, width), 1)
    place = lax.broadcasted_iota(jnp.int32, (peers, width), 1)
    peer = lax.broadcasted_iota(jnp.int32, (peers, width), 0)
    mine = (place >> 2) == peer
    top = shared.astype(jnp.bfloat16)
    rest = (shared - top.astype(jnp.float32)).astype(jnp.bfloat16)
    for dim in range(3):
        choose = (source == 64 + 3 * (target & 3) + dim).astype(jnp.float32).astype(jnp.bfloat16)
        value = jnp.dot(top, choose, preferred_element_type=jnp.float32) + jnp.dot(
            rest, choose, preferred_element_type=jnp.float32
        )
        row = jnp.sum(jnp.where(mine, value, 0.0), axis=0, keepdims=True)
        cells[dim : dim + 1, :] = row.astype(jnp.int32) - 1


def vmem():
    return pl.BlockSpec(memory_space=pltpu.VMEM)


def prepare(own, low_y, high_y, low_z, high_z, offsets, peers):
    _, rows_y, rows_z, lanes = own.shape
    _, blocks, tracers = offsets.shape
    halves = tracers // lanes
    return pl.pallas_call(
        prepare_kernel,
        out_shape=(
            jax.ShapeDtypeStruct(((rows_y + 2 * HALO) * (rows_z + 2 * HALO) * 16 + 64, lanes), jnp.float32),
            jax.ShapeDtypeStruct((3, halves, blocks * 8 + 8, lanes), jnp.float32),
            jax.ShapeDtypeStruct((peers, halves * 3 * CAP + 1, 1, lanes), jnp.float32),
        ),
        in_specs=[vmem()] * 6,
        out_specs=(vmem(), vmem(), vmem()),
        compiler_params=pltpu.CompilerParams(vmem_limit_bytes=40 * 1024 * 1024),
        cost_estimate=pl.CostEstimate(flops=30_000_000, bytes_accessed=8_000_000, transcendentals=0),
        name="prepare",
    )(own, low_y, high_y, low_z, high_z, offsets)


def advance(live_counts, table, corners, offsets, traits, cell_rows, prepared):
    lanes = corners[0].shape[-1]
    _, blocks, tracers = offsets.shape
    halves = tracers // lanes
    return pl.pallas_call(
        advance_kernel,
        out_shape=tuple(jax.ShapeDtypeStruct(x.shape, x.dtype) for x in prepared),
        in_specs=[pl.BlockSpec(memory_space=pltpu.SMEM), pl.BlockSpec(memory_space=pl.ANY)] + [vmem()] * 8,
        out_specs=(vmem(), vmem(), vmem()),
        input_output_aliases={7: 0, 8: 1, 9: 2},
        scratch_shapes=[
            pltpu.VMEM((halves, blocks * 16 + 16, lanes), jnp.float32),
            pltpu.VMEM((halves, blocks * 16 + 16, lanes), jnp.float32),
            pltpu.SMEM(table.shape, jnp.int32),
            pltpu.SemaphoreType.DMA,
        ],
        compiler_params=pltpu.CompilerParams(vmem_limit_bytes=40 * 1024 * 1024),
        name="advance",
    )(live_counts, table, *corners, offsets, traits, cell_rows, *prepared)[2]


def unpack(received, peers, rows_y, tracers):
    _, per, _, lanes = received.shape
    part = peers // UNPACK_STEPS
    return pl.pallas_call(
        lambda *refs: unpack_kernel(*refs, scale=1.0 / (tracers * peers)),
        grid=(UNPACK_STEPS,),
        out_shape=(
            jax.ShapeDtypeStruct((4, rows_y), jnp.float32),
            jax.ShapeDtypeStruct((3, peers * CAP, tracers), jnp.float32),
            jax.ShapeDtypeStruct((3, peers * CAP), jnp.int32),
        ),
        in_specs=[pl.BlockSpec((part, per, 1, lanes), lambda i: (i, 0, 0, 0))],
        out_specs=(
            pl.BlockSpec((4, rows_y), lambda i: (0, 0)),
            pl.BlockSpec((3, part * CAP, tracers), lambda i: (0, i, 0)),
            pl.BlockSpec((3, part * CAP), lambda i: (0, i)),
        ),
        scratch_shapes=[
            pltpu.VMEM((3 * tracers // lanes, part * CAP, lanes), jnp.float32),
            pltpu.VMEM((part, lanes), jnp.float32),
        ],
        name="unpack",
    )(received)


def neighbour(x, axis, step, name):
    count = lax.axis_size(axis)
    with jax.named_scope(name):
        return lax.ppermute(x, axis, [(i, (i + step) % count) for i in range(count)])


def halo(flow_field):
    rows_y, rows_z = flow_field.shape[1:3]
    by_z = jnp.swapaxes(flow_field, 1, 2)
    low_y = neighbour(flow_field[:, rows_y - HALO :], "wide", 1, "low_y")
    high_y = neighbour(flow_field[:, :HALO], "wide", -1, "high_y")
    low_z = neighbour(by_z[:, rows_z - HALO :], "narrow", 1, "low_z")
    high_z = neighbour(by_z[:, :HALO], "narrow", -1, "high_z")

    def corners(start):
        piece = jnp.concatenate([low_y[:, :, start : start + HALO], high_y[:, :, start : start + HALO]], axis=1)
        return jnp.transpose(piece, (2, 0, 1, 3)).reshape(HALO, -1, piece.shape[3])

    low_corners = neighbour(corners(rows_z - HALO), "narrow", 1, "low_corners")
    high_corners = neighbour(corners(0), "narrow", -1, "high_corners")
    return (flow_field, low_y, high_y, low_z, high_z), (low_corners, high_corners)


def plan(cells_first, cells_second, destination, extents, first_y, first_z, lanes):
    blocks = cells_first.shape[1]
    index = jnp.arange(blocks, dtype=jnp.int32)

    def tile(cells):
        ly = (cells[1] - first_y + HALO) % extents[1]
        lz = (cells[2] - first_z + HALO) % extents[2]
        return [ly, lz, (cells[0] + SLOT * (ly & 7)) & (lanes - 1)]

    shift = [
        (cells_first[d] - cells_second[d] + extents[d] // 2) % extents[d] - extents[d] // 2 for d in range(3)
    ]
    target = destination[0]
    same = (target[:, None] == target[None, :]) & (index[None, :] < index[:, None])
    rank = jnp.sum(same.astype(jnp.int32), axis=1)
    table = jnp.stack(
        tile(cells_first)
        + tile(cells_second)
        + [target, rank]
    )
    lane = jnp.arange(lanes, dtype=jnp.int32)[None, :]
    column = (cells_first[1] + 2 - first_y) % extents[1]
    traits = jnp.where((lane < 64) & ((lane & 15) == column[:, None]), 1.0, 0.0)
    for d in range(3):
        traits = jnp.where(lane == 64 + d, shift[d].astype(jnp.float32)[:, None], traits)
    place = lane - 64 - 3 * rank[:, None]
    cell = jnp.where(place == 0, cells_first[0][:, None], jnp.where(place == 1, cells_first[1][:, None], cells_first[2][:, None]))
    cell_rows = jnp.where((place >= 0) & (place < 3), (cell + 1).astype(jnp.float32), 0.0)
    return table, traits, cell_rows


def local(flow_field, offsets, cells_first, cells_second, live_counts, destination):
    wide_count = lax.axis_size("wide")
    narrow_count = lax.axis_size("narrow")
    _, rows_y, rows_z, rows_x = flow_field.shape
    tracers = offsets.shape[2]
    assert rows_z + 2 * HALO == EXT_Z
    pieces, corners = halo(flow_field)
    offsets = jnp.swapaxes(offsets, 0, 1)
    prepared = prepare(*pieces, offsets, narrow_count)
    table, traits, cell_rows = plan(
        cells_first.T, cells_second.T, destination.T,
        (rows_x, rows_y * wide_count, rows_z * narrow_count),
        lax.axis_index("wide") * rows_y, lax.axis_index("narrow") * rows_z, rows_x,
    )
    sent = advance(live_counts, table, corners, offsets, traits, cell_rows, prepared)
    received = lax.all_to_all(sent, "narrow", split_axis=0, concat_axis=0, tiled=True)
    profile, moved, cells = unpack(received, narrow_count, rows_y, tracers)
    return profile, jnp.swapaxes(moved, 0, 1), cells.T


def solution(mesh):
    return jax.shard_map(
        local,
        mesh=mesh,
        in_specs=(
            P(None, "wide", "narrow", None),
            P(("wide", "narrow"), None, None),
            P(("wide", "narrow"), None),
            P(("wide", "narrow"), None),
            P(("wide", "narrow")),
            P(("wide", "narrow"), None),
        ),
        out_specs=(P(None, "wide"), P(("wide", "narrow"), None, None), P(("wide", "narrow"), None)),
        check_vma=False,
    )
```
